32 devices in a mesh: dp: 1 (over z), tp: 4 (over y), sp: 8 (over x, core).
Axes of the slice: x: 4, y: 4, z: 1, core: 2. Of those that a mesh axis runs over, the one named last changes fastest.
The devices are a block of a 4x4x8 slice.
Arguments:
- layer_in: bfloat16 [128, 6144], P('dp')
- new_pos: int32 [128], P('dp')
- k_cache: bfloat16 [128, 512, 8, 128], P('dp', 'sp', 'tp')
- v_cache: bfloat16 [128, 512, 8, 128], P('dp', 'sp', 'tp')
- attn_gain: bfloat16 [6144], replicated
- w_query: bfloat16 [6144, 6144], P(None, 'tp')
- w_key: bfloat16 [6144, 1024], P(None, 'tp')
- w_value: bfloat16 [6144, 1024], P(None, 'tp')
- w_out: bfloat16 [6144, 6144], P('tp')
- mlp_gain: bfloat16 [6144], replicated
- w_gate: bfloat16 [6144, 16384], P(None, 'tp')
- w_up: bfloat16 [6144, 16384], P(None, 'tp')
- w_down: bfloat16 [16384, 6144], P('tp')
Outputs:
- output 1: bfloat16 [128, 6144], P('dp')
- output 2: bfloat16 [128, 512, 8, 128], P('dp', 'sp', 'tp')
- output 3: bfloat16 [128, 512, 8, 128], P('dp', 'sp', 'tp')
- output 4: bfloat16 [128, 8, 128], P('dp', 'tp')
- output 5: bfloat16 [128, 8, 128], P('dp', 'tp')
All inputs are finite; a program needn't handle non-finite values.
Results may differ from the reference program's by a relative error of at most 0.00516591.
Values sent between devices are 32-bit elements.
A program may use at most 768 MiB of HBM per device.

```python
import jax
import jax.numpy as jnp
from jax import lax

BATCH_ROWS = 128
CACHE_LEN = 512
MODEL_DIM = 6144
NUM_HEADS = 48
KV_HEADS = 8
HEAD_DIM = 128
FFN_DIM = 16384
ROPE_THETA = 1000000
COARSE_GROUPS = 64
GROUP_SIZE = NUM_HEADS // KV_HEADS
SCORE_SCALE = HEAD_DIM ** -0.5
MIN_POS = CACHE_LEN // 16


def weight(key_w, w_shape, fan_in):
    return (jax.random.normal(key_w, w_shape, jnp.float32) * fan_in ** -0.5).astype(jnp.bfloat16)


def setup_inputs(seed: int = 0, part: int = 0) -> dict:
    part_key = jax.random.fold_in(jax.random.key(seed), part)
    row_keys = jax.random.split(part_key, 7)
    w_keys = jax.random.split(jax.random.key(seed + 1), 9)
    layer_in = jax.random.normal(row_keys[0], (BATCH_ROWS, MODEL_DIM), jnp.float32).astype(jnp.bfloat16)
    pos_draw = jax.random.randint(row_keys[1], (BATCH_ROWS,), MIN_POS, CACHE_LEN)
    new_pos = jnp.where(jnp.arange(BATCH_ROWS) == 0, CACHE_LEN - 1, pos_draw).astype(jnp.int32)
    cache_shape = (BATCH_ROWS, CACHE_LEN, KV_HEADS, HEAD_DIM)
    coarse_shape = (BATCH_ROWS, COARSE_GROUPS, 1, KV_HEADS, HEAD_DIM)
    span_shape = (BATCH_ROWS, COARSE_GROUPS, CACHE_LEN // COARSE_GROUPS, KV_HEADS, HEAD_DIM)
    k_coarse = jnp.broadcast_to(jax.random.normal(row_keys[2], coarse_shape, jnp.float32), span_shape).reshape(cache_shape)
    v_coarse = jnp.broadcast_to(jax.random.normal(row_keys[3], coarse_shape, jnp.float32), span_shape).reshape(cache_shape)
    k_cache = (jax.random.normal(row_keys[4], cache_shape, jnp.float32) + 1.5 * k_coarse).astype(jnp.bfloat16)
    v_cache = (0.5 * jax.random.normal(row_keys[5], cache_shape, jnp.float32) + 2.0 * v_coarse).astype(jnp.bfloat16)
    attn_gain = (1.0 + 0.2 * jax.random.normal(w_keys[0], (MODEL_DIM,), jnp.float32)).astype(jnp.bfloat16)
    mlp_gain = (1.0 + 0.2 * jax.random.normal(w_keys[1], (MODEL_DIM,), jnp.float32)).astype(jnp.bfloat16)
    return {
        'layer_in': layer_in,
        'new_pos': new_pos,
        'k_cache': k_cache,
        'v_cache': v_cache,
        'attn_gain': attn_gain,
        'w_query': weight(w_keys[2], (MODEL_DIM, NUM_HEADS * HEAD_DIM), MODEL_DIM),
        'w_key': weight(w_keys[3], (MODEL_DIM, KV_HEADS * HEAD_DIM), MODEL_DIM),
        'w_value': weight(w_keys[4], (MODEL_DIM, KV_HEADS * HEAD_DIM), MODEL_DIM),
        'w_out': weight(w_keys[5], (NUM_HEADS * HEAD_DIM, MODEL_DIM), NUM_HEADS * HEAD_DIM),
        'mlp_gain': mlp_gain,
        'w_gate': weight(w_keys[6], (MODEL_DIM, FFN_DIM), MODEL_DIM),
        'w_up': weight(w_keys[7], (MODEL_DIM, FFN_DIM), MODEL_DIM),
        'w_down': weight(w_keys[8], (FFN_DIM, MODEL_DIM), FFN_DIM),
    }


def rms_norm(in_vec, gain_vec):
    mean_sq = jnp.mean(jnp.square(in_vec), axis=-1, keepdims=True)
    return in_vec * lax.rsqrt(mean_sq + 1e-5) * gain_vec.astype(jnp.float32)


def apply_rotary(in_vec, positions):
    half_idx = jnp.arange(HEAD_DIM // 2, dtype=jnp.float32)
    inv_freq = 1.0 / (ROPE_THETA ** (2.0 * half_idx / HEAD_DIM))
    angles = positions.astype(jnp.float32)[:, None] * inv_freq[None, :]
    cos_a = jnp.cos(angles)[:, None, :]
    sin_a = jnp.sin(angles)[:, None, :]
    pair_view = in_vec.reshape(in_vec.shape[:-1] + (HEAD_DIM // 2, 2))
    even_part = pair_view[..., 0]
    odd_part = pair_view[..., 1]
    rotated = jnp.stack([even_part * cos_a - odd_part * sin_a, even_part * sin_a + odd_part * cos_a], axis=-1)
    return rotated.reshape(in_vec.shape)


def reference(layer_in, new_pos, k_cache, v_cache, attn_gain, w_query, w_key, w_value, w_out, mlp_gain, w_gate, w_up, w_down):
    x_f32 = layer_in.astype(jnp.float32)
    normed = rms_norm(x_f32, attn_gain).astype(jnp.bfloat16)
    q_proj = jnp.dot(normed, w_query, preferred_element_type=jnp.float32).reshape(BATCH_ROWS, NUM_HEADS, HEAD_DIM)
    k_proj = jnp.dot(normed, w_key, preferred_element_type=jnp.float32).reshape(BATCH_ROWS, KV_HEADS, HEAD_DIM)
    v_new = jnp.dot(normed, w_value, preferred_element_type=jnp.float32).reshape(BATCH_ROWS, KV_HEADS, HEAD_DIM).astype(jnp.bfloat16)
    q_rot = apply_rotary(q_proj, new_pos).astype(jnp.bfloat16)
    k_rot = apply_rotary(k_proj, new_pos).astype(jnp.bfloat16)
    slot_ids = jnp.arange(CACHE_LEN)

    def one_row(row_args):
        q_row, k_row, v_row, k_rows, v_rows, pos_row = row_args
        is_new = (slot_ids == pos_row)[:, None, None]
        k_upd = jnp.where(is_new, k_row[None], k_rows)
        v_upd = jnp.where(is_new, v_row[None], v_rows)
        q_grp = q_row.reshape(KV_HEADS, GROUP_SIZE, HEAD_DIM).astype(jnp.float32)
        scores = jnp.einsum('kgd,skd->kgs', q_grp, k_upd.astype(jnp.float32)) * SCORE_SCALE
        scores = jnp.where(slot_ids <= pos_row, scores, -jnp.inf)
        row_max = jnp.max(scores, axis=-1, keepdims=True)
        prob_vals = jnp.exp(scores - row_max)
        denom_sum = jnp.sum(prob_vals, axis=-1)
        weighted = jnp.einsum('kgs,skd->kgd', prob_vals.astype(jnp.bfloat16).astype(jnp.float32), v_upd.astype(jnp.float32))
        attn_row = (weighted / denom_sum[..., None]).reshape(NUM_HEADS * HEAD_DIM)
        return attn_row, k_upd, v_upd

    attn_rows, k_out, v_out = lax.map(one_row, (q_rot, k_rot, v_new, k_cache, v_cache, new_pos))
    attn_vec = attn_rows.astype(jnp.bfloat16)
    hidden = x_f32 + jnp.dot(attn_vec, w_out, preferred_element_type=jnp.float32)
    normed_mlp = rms_norm(hidden, mlp_gain).astype(jnp.bfloat16)
    gate_pre = jnp.dot(normed_mlp, w_gate, preferred_element_type=jnp.float32)
    up_proj = jnp.dot(normed_mlp, w_up, preferred_element_type=jnp.float32)
    act_bf = (jax.nn.silu(gate_pre) * up_proj).astype(jnp.bfloat16)
    layer_out = (hidden + jnp.dot(act_bf, w_down, preferred_element_type=jnp.float32)).astype(jnp.bfloat16)
    return (layer_out, k_out, v_out, k_rot, v_new)
```

```python
import functools

import numpy as np
import jax
import jax.numpy as jnp
from jax import lax
from jax.experimental import pallas as pl
from jax.experimental.pallas import tpu as pltpu
from jax.sharding import PartitionSpec as P

ROPE_THETA = 1000000
EPS = 1e-5
NEG = -1e30
LANES = 128
HEAD_PAD = 16
WCHUNK = 256
BLK_ROWS = 16
UNROLL = 8

ANY = pl.BlockSpec(memory_space=pl.ANY)
VM = pl.BlockSpec(memory_space=pltpu.VMEM)


def attn_kernel(pos, x_ref, gain_ref, freq_ref, wq, wk, wv, kc, vc, o_out, kc_out, vc_out, kn_out, vn_out,
                xn, wbuf, kbuf, vbuf, ang, qs, kns, vns, osc, msc, lsc, wsem, csem, osem, *, blk_len, heads, kv_loc):
    rows, _ = x_ref.shape
    hd = LANES
    group = heads // kv_loc
    n_q = wq.shape[1] // WCHUNK
    per_row = blk_len * kv_loc
    n_blk = rows // BLK_ROWS
    blk_sz = BLK_ROWS * per_row

    def w_copy(i):
        if i == 0:
            src = wk
        elif i == 1:
            src = wv
        else:
            src = wq.at[:, pl.ds((i - 2) * WCHUNK, WCHUNK)]
        return pltpu.make_async_copy(src, wbuf.at[i], wsem.at[i])

    def c_in(j):
        sl = pl.ds(j * blk_sz, blk_sz)
        return (pltpu.make_async_copy(kc.at[sl], kbuf.at[sl], csem.at[2 * j]),
                pltpu.make_async_copy(vc.at[sl], vbuf.at[sl], csem.at[2 * j + 1]))

    def c_out(j):
        sl = pl.ds(j * blk_sz, blk_sz)
        return (pltpu.make_async_copy(kbuf.at[sl], kc_out.at[sl], osem.at[2 * j]),
                pltpu.make_async_copy(vbuf.at[sl], vc_out.at[sl], osem.at[2 * j + 1]))

    for i in range(n_q + 2):
        w_copy(i).start()
    for j in range(n_blk):
        for c in c_in(j):
            c.start()

    gain = gain_ref[...].astype(jnp.float32)
    for r in range(0, rows, 16):
        x = x_ref[r:r + 16, :].astype(jnp.float32)
        ms = jnp.mean(x * x, axis=-1, keepdims=True)
        xn[r:r + 16, :] = (x * lax.rsqrt(ms + EPS) * gain).astype(jnp.bfloat16)

    def ang_body(g, _):
        for u in range(8):
            b = g * 8 + u
            ang[pl.ds(b, 1), :] = pos[b].astype(jnp.float32) * freq_ref[...]
        return 0
    lax.fori_loop(0, rows // 8, ang_body, 0)
    lane = lax.broadcasted_iota(jnp.int32, (rows, hd), 1)
    even = lax.rem(lane, 2) == 0
    cos_a = jnp.cos(ang[...])
    sin_a = jnp.sin(ang[...])
    ang[...] = cos_a
    msc[0:rows, :] = jnp.where(even, -sin_a, sin_a)

    def rope(v):
        swapped = jnp.where(even, pltpu.roll(v, hd - 1, 1), pltpu.roll(v, 1, 1))
        return v * ang[...] + swapped * msc[0:rows, :]

    qs[...] = jnp.zeros(qs.shape, jnp.float32)

    w_copy(0).wait()
    res = jnp.dot(xn[...], wbuf[0], preferred_element_type=jnp.float32)
    for h in range(kv_loc):
        kns[pl.ds(h, rows, stride=kv_loc), :] = rope(res[:, h * hd:(h + 1) * hd]).astype(jnp.bfloat16).astype(jnp.float32)
    w_copy(1).wait()
    res = jnp.dot(xn[...], wbuf[1], preferred_element_type=jnp.float32)
    for h in range(kv_loc):
        vns[pl.ds(h, rows, stride=kv_loc), :] = res[:, h * hd:(h + 1) * hd].astype(jnp.bfloat16).astype(jnp.float32)
    kn_out[...] = kns[...].astype(jnp.bfloat16)
    vn_out[...] = vns[...].astype(jnp.bfloat16)

    per_w = WCHUNK // hd

    def q_body(i, _):
        pltpu.make_async_copy(wq.at[:, pl.ds(0, WCHUNK)], wbuf.at[i + 2], wsem.at[i + 2]).wait()
        r = jnp.dot(xn[...], wbuf[i + 2], preferred_element_type=jnp.float32)
        for h in range(per_w):
            qs[pl.ds(i * per_w + h, rows, stride=HEAD_PAD), :] = rope(r[:, h * hd:(h + 1) * hd])
        return 0
    lax.fori_loop(0, n_q, q_body, 0)

    base = lax.axis_index('sp') * blk_len
    s_lane = lax.broadcasted_iota(jnp.int32, (HEAD_PAD, per_row), 1)
    s_head = lax.broadcasted_iota(jnp.int32, (HEAD_PAD, per_row), 0)
    own = lax.rem(s_lane, kv_loc) == lax.div(s_head, group)
    slot_rel = jnp.where(own, lax.div(s_lane, kv_loc), 1 << 20)
    u_row = lax.broadcasted_iota(jnp.int32, (16, hd), 0)
    u_slot = lax.div(u_row, kv_loc)
    u_first = lax.rem(u_row, kv_loc) == 0
    scale = hd ** -0.5
    slots16 = 16 // kv_loc

    def blk_body(j, _):
        sl = pl.ds(pl.multiple_of(j * blk_sz, blk_sz), blk_sz)
        pltpu.make_async_copy(kc.at[sl], kbuf.at[sl], csem.at[2 * j]).wait()
        pltpu.make_async_copy(vc.at[sl], vbuf.at[sl], csem.at[2 * j + 1]).wait()

        def b_body(g, _):
            for u in range(UNROLL):
                b = j * BLK_ROWS + g * UNROLL + u
                rel = pos[b] - base
                relc = jnp.clip(rel, 0, blk_len - 1)
                grp = lax.div(relc, slots16)
                start = pl.multiple_of(b * per_row + grp * 16, 16)
                hit = u_slot == (rel - grp * slots16)
                for new, buf in ((kns, kbuf), (vns, vbuf)):
                    n0 = new[pl.ds(b * kv_loc, 1), :]
                    n1 = new[pl.ds(b * kv_loc + 1, 1), :]
                    old = buf[pl.ds(start, 16), :].astype(jnp.float32)
                    buf[pl.ds(start, 16), :] = jnp.where(hit, jnp.where(u_first, n0, n1), old).astype(jnp.bfloat16)
            for u in range(UNROLL):
                b = j * BLK_ROWS + g * UNROLL + u
                rel = pos[b] - base
                kb = kbuf[pl.ds(pl.multiple_of(b * per_row, per_row), per_row), :]
                vb = vbuf[pl.ds(pl.multiple_of(b * per_row, per_row), per_row), :]
                qb = qs[pl.ds(pl.multiple_of(b * HEAD_PAD, HEAD_PAD), HEAD_PAD), :].astype(jnp.bfloat16)
                s = lax.dot_general(qb, kb, (((1,), (1,)), ((), ())), preferred_element_type=jnp.float32) * scale
                valid = slot_rel <= rel
                s = jnp.where(valid, s, NEG)
                m = jnp.max(s, axis=-1, keepdims=True)
                w = jnp.where(valid, jnp.exp(s - m), 0.0)
                l = jnp.sum(w, axis=-1, keepdims=True)
                o = jnp.dot(w.astype(jnp.bfloat16), vb, preferred_element_type=jnp.float32)
                rs = pl.ds(pl.multiple_of(b * HEAD_PAD, HEAD_PAD), HEAD_PAD)
                osc[rs, :] = o
                msc[rs, :] = jnp.broadcast_to(m, (HEAD_PAD, hd))
                lsc[rs, :] = jnp.broadcast_to(l, (HEAD_PAD, hd))
            return 0
        lax.fori_loop(0, BLK_ROWS // UNROLL, b_body, 0)
        pltpu.make_async_copy(kbuf.at[sl], kc_out.at[sl], osem.at[2 * j]).start()
        pltpu.make_async_copy(vbuf.at[sl], vc_out.at[sl], osem.at[2 * j + 1]).start()
        return 0
    lax.fori_loop(0, n_blk, blk_body, 0)

    st = jnp.zeros((rows, hd), jnp.float32)
    for h in range(heads):
        o_out[:, h * hd:(h + 1) * hd] = osc[pl.ds(h, rows, stride=HEAD_PAD), :]
        st = jnp.where(lane == h, msc[pl.ds(h, rows, stride=HEAD_PAD), :], st)
        st = jnp.where(lane == HEAD_PAD + h, lsc[pl.ds(h, rows, stride=HEAD_PAD), :], st)
    o_out[:, heads * hd:] = st
    for j in range(n_blk):
        for c in c_out(j):
            c.wait()


def attn_call(pos, x, gain, wq, wk, wv, kc, vc, *, blk_len, heads, kv_loc):
    rows, dim = x.shape
    hd = LANES
    half = np.arange(hd) // 2
    freq = jnp.asarray((1.0 / (float(ROPE_THETA) ** (2.0 * half / hd))).astype(np.float32)).reshape(1, hd)
    n_q = wq.shape[1] // WCHUNK
    n_blk = rows // BLK_ROWS
    crow = kc.shape[0]
    f32, bf = jnp.float32, jnp.bfloat16
    return pl.pallas_call(
        functools.partial(attn_kernel, blk_len=blk_len, heads=heads, kv_loc=kv_loc),
        out_shape=(jax.ShapeDtypeStruct((rows, heads * hd + LANES), f32), jax.ShapeDtypeStruct(kc.shape, bf),
                   jax.ShapeDtypeStruct(vc.shape, bf), jax.ShapeDtypeStruct((rows * kv_loc, hd), bf),
                   jax.ShapeDtypeStruct((rows * kv_loc, hd), bf)),
        in_specs=[pl.BlockSpec(memory_space=pltpu.SMEM), VM, VM, VM, ANY, ANY, ANY, ANY, ANY],
        out_specs=(VM, ANY, ANY, VM, VM),
        scratch_shapes=[
            pltpu.VMEM((rows, dim), bf), pltpu.VMEM((n_q + 2, dim, WCHUNK), bf),
            pltpu.VMEM((crow, hd), bf), pltpu.VMEM((crow, hd), bf),
            pltpu.VMEM((rows, hd), f32), pltpu.VMEM((rows * HEAD_PAD, hd), f32),
            pltpu.VMEM((rows * kv_loc, hd), f32), pltpu.VMEM((rows * kv_loc, hd), f32),
            pltpu.VMEM((rows * HEAD_PAD, hd), f32), pltpu.VMEM((rows * HEAD_PAD, hd), f32),
            pltpu.VMEM((rows * HEAD_PAD, hd), f32),
            pltpu.SemaphoreType.DMA((n_q + 2,)), pltpu.SemaphoreType.DMA((2 * n_blk,)),
            pltpu.SemaphoreType.DMA((2 * n_blk,)),
        ],
        compiler_params=pltpu.CompilerParams(vmem_limit_bytes=60 * 1024 * 1024),
        name='attn',
    )(pos, x, gain.reshape(1, dim), freq, wq, wk, wv, kc, vc)


def rms_norm(in_vec, gain_vec):
    mean_sq = jnp.mean(jnp.square(in_vec), axis=-1, keepdims=True)
    return in_vec * lax.rsqrt(mean_sq + EPS) * gain_vec.astype(jnp.float32)


def solution(mesh):
    def local_step(layer_in, new_pos, k_blk, v_blk, attn_gain, w_query, w_key, w_value, w_out, mlp_gain, w_gate, w_up, w_down):
        num_rows = layer_in.shape[0]
        blk_len, kv_loc, head_dim = k_blk.shape[1:]
        heads = w_query.shape[1] // head_dim
        flat = (num_rows * blk_len * kv_loc, head_dim)
        part, k_upd, v_upd, k_new, v_new = attn_call(
            new_pos, layer_in, attn_gain, w_query, w_key, w_value, k_blk.reshape(flat), v_blk.reshape(flat),
            blk_len=blk_len, heads=heads, kv_loc=kv_loc)
        o_part = part[:, :heads * head_dim].reshape(num_rows, heads, head_dim)
        m_loc = part[:, heads * head_dim:heads * head_dim + heads]
        l_loc = part[:, heads * head_dim + HEAD_PAD:heads * head_dim + HEAD_PAD + heads]
        m_all = lax.pmax(m_loc, 'sp')
        fac = jnp.exp(m_loc - m_all)
        denom = lax.psum(l_loc * fac, 'sp')
        weighted = lax.psum(o_part * fac[:, :, None], 'sp')
        attn_vec = (weighted / denom[:, :, None]).reshape(num_rows, heads * head_dim).astype(jnp.bfloat16)
        x_f32 = layer_in.astype(jnp.float32)
        hidden = x_f32 + lax.psum(jnp.dot(attn_vec, w_out, preferred_element_type=jnp.float32), 'tp')
        normed_mlp = rms_norm(hidden, mlp_gain).astype(jnp.bfloat16)
        gate_pre = jnp.dot(normed_mlp, w_gate, preferred_element_type=jnp.float32)
        up_proj = jnp.dot(normed_mlp, w_up, preferred_element_type=jnp.float32)
        act_bf = (jax.nn.silu(gate_pre) * up_proj).astype(jnp.bfloat16)
        mlp_part = jnp.dot(act_bf, w_down, preferred_element_type=jnp.float32)
        layer_out = (hidden + lax.psum(mlp_part, 'tp')).astype(jnp.bfloat16)
        new_shape = (num_rows, kv_loc, head_dim)
        return layer_out, k_upd.reshape(k_blk.shape), v_upd.reshape(v_blk.shape), k_new.reshape(new_shape), v_new.reshape(new_shape)

    cache_spec = P('dp', 'sp', 'tp', None)
    new_spec = P('dp', 'tp', None)
    in_specs = (P('dp', None), P('dp'), cache_spec, cache_spec, P(None), P(None, 'tp'), P(None, 'tp'), P(None, 'tp'), P('tp', None), P(None), P(None, 'tp'), P(None, 'tp'), P('tp', None))
    out_specs = (P('dp', None), cache_spec, cache_spec, new_spec, new_spec)
    return jax.shard_map(local_step, mesh=mesh, in_specs=in_specs, out_specs=out_specs, check_vma=False)
```

```python
import functools

import numpy as np
import jax
import jax.numpy as jnp
from jax import lax
from jax.experimental import pallas as pl
from jax.experimental.pallas import tpu as pltpu
from jax.sharding import PartitionSpec as P

ROPE_THETA = 1000000
EPS = 1e-5
NEG = -1e30
LANES = 128
HEAD_PAD = 16
KCH = 512
BLK_ROWS = 16
UNROLL = 8

ANY = pl.BlockSpec(memory_space=pl.ANY)
VM = pl.BlockSpec(memory_space=pltpu.VMEM)


def attn_kernel(pos, x_ref, gain_ref, freq_ref, wq, wk, wv, kc, vc, o_out, kc_out, vc_out, kn_out, vn_out,
                xn, wqb, wkb, wvb, acc, kbuf, vbuf, ang, qs, kns, vns, osc, msc, lsc, wsem, csem, osem, *, blk_len, heads, kv_loc):
    rows, _ = x_ref.shape
    hd = LANES
    group = heads // kv_loc
    n_k = wq.shape[0] // KCH
    qw, kw = wq.shape[1], wk.shape[1]
    per_row = blk_len * kv_loc
    n_blk = rows // BLK_ROWS
    blk_sz = BLK_ROWS * per_row

    def w_copies(k):
        r = pl.ds(pl.multiple_of(k * KCH, KCH), KCH)
        return [pltpu.make_async_copy(w.at[r], buf.at[r], wsem.at[k, i]) for i, (w, buf) in enumerate(((wq, wqb), (wk, wkb), (wv, wvb)))]

    def c_in(j):
        sl = pl.ds(j * blk_sz, blk_sz)
        return (pltpu.make_async_copy(kc.at[sl], kbuf.at[sl], csem.at[2 * j]),
                pltpu.make_async_copy(vc.at[sl], vbuf.at[sl], csem.at[2 * j + 1]))

    def c_out(j):
        sl = pl.ds(j * blk_sz, blk_sz)
        return (pltpu.make_async_copy(kbuf.at[sl], kc_out.at[sl], osem.at[2 * j]),
                pltpu.make_async_copy(vbuf.at[sl], vc_out.at[sl], osem.at[2 * j + 1]))

    for k in range(n_k):
        for cp in w_copies(k):
            cp.start()
    for j in range(n_blk):
        for c in c_in(j):
            c.start()

    gain = gain_ref[...].astype(jnp.float32)
    gain = jnp.concatenate([gain[j:j + 1, :] for j in range(gain.shape[0])], axis=1)
    for r in range(0, rows, 16):
        x = x_ref[r:r + 16, :].astype(jnp.float32)
        ms = jnp.mean(x * x, axis=-1, keepdims=True)
        xn[r:r + 16, :] = (x * lax.rsqrt(ms + EPS) * gain).astype(jnp.bfloat16)

    def ang_body(g, _):
        for u in range(8):
            b = g * 8 + u
            ang[pl.ds(b, 1), :] = pos[b].astype(jnp.float32) * freq_ref[...]
        return 0
    lax.fori_loop(0, rows // 8, ang_body, 0)
    lane = lax.broadcasted_iota(jnp.int32, (rows, hd), 1)
    even = lax.rem(lane, 2) == 0
    cos_a = jnp.cos(ang[...])
    sin_a = jnp.sin(ang[...])
    ang[...] = cos_a
    msc[0:rows, :] = jnp.where(even, -sin_a, sin_a)

    def rope(v):
        swapped = jnp.where(even, pltpu.roll(v, hd - 1, 1), pltpu.roll(v, 1, 1))
        return v * ang[...] + swapped * msc[0:rows, :]

    qs[...] = jnp.zeros(qs.shape, jnp.float32)

    acc[...] = jnp.zeros(acc.shape, jnp.float32)

    def w_body(k, _):
        r = pl.ds(pl.multiple_of(k * KCH, KCH), KCH)
        cps = w_copies(k)
        lhs = xn[:, r]
        cps[0].wait()
        acc[:, 0:qw] += jnp.dot(lhs, wqb[r, :], preferred_element_type=jnp.float32)
        cps[1].wait()
        acc[:, qw:qw + kw] += jnp.dot(lhs, wkb[r, :], preferred_element_type=jnp.float32)
        cps[2].wait()
        acc[:, qw + kw:] += jnp.dot(lhs, wvb[r, :], preferred_element_type=jnp.float32)
        return 0
    lax.fori_loop(0, n_k, w_body, 0)
    for h in range(kv_loc):
        o = qw + h * hd
        kns[pl.ds(h, rows, stride=kv_loc), :] = rope(acc[:, o:o + hd]).astype(jnp.bfloat16).astype(jnp.float32)
        o = qw + kw + h * hd
        vns[pl.ds(h, rows, stride=kv_loc), :] = acc[:, o:o + hd].astype(jnp.bfloat16).astype(jnp.float32)
    kn_out[...] = kns[...].astype(jnp.bfloat16)
    vn_out[...] = vns[...].astype(jnp.bfloat16)
    for h in range(heads):
        qs[pl.ds(h, rows, stride=HEAD_PAD), :] = rope(acc[:, h * hd:(h + 1) * hd])

    base = lax.axis_index('sp') * blk_len
    s_lane = lax.broadcasted_iota(jnp.int32, (HEAD_PAD, per_row), 1)
    s_head = lax.broadcasted_iota(jnp.int32, (HEAD_PAD, per_row), 0)
    own = lax.rem(s_lane, kv_loc) == lax.div(s_head, group)
    slot_rel = jnp.where(own, lax.div(s_lane, kv_loc), 1 << 20)
    u_row = lax.broadcasted_iota(jnp.int32, (16, hd), 0)
    u_slot = lax.div(u_row, kv_loc)
    u_first = lax.rem(u_row, kv_loc) == 0
    scale = hd ** -0.5
    slots16 = 16 // kv_loc

    def blk_body(j, _):
        sl = pl.ds(pl.multiple_of(j * blk_sz, blk_sz), blk_sz)
        pltpu.make_async_copy(kc.at[sl], kbuf.at[sl], csem.at[2 * j]).wait()
        pltpu.make_async_copy(vc.at[sl], vbuf.at[sl], csem.at[2 * j + 1]).wait()

        def b_body(g, _):
            for u in range(UNROLL):
                b = j * BLK_ROWS + g * UNROLL + u
                rel = pos[b] - base
                relc = jnp.clip(rel, 0, blk_len - 1)
                grp = lax.div(relc, slots16)
                start = pl.multiple_of(b * per_row + grp * 16, 16)
                hit = u_slot == (rel - grp * slots16)
                for new, buf in ((kns, kbuf), (vns, vbuf)):
                    n0 = new[pl.ds(b * kv_loc, 1), :]
                    n1 = new[pl.ds(b * kv_loc + 1, 1), :]
                    old = buf[pl.ds(start, 16), :].astype(jnp.float32)
                    buf[pl.ds(start, 16), :] = jnp.where(hit, jnp.where(u_first, n0, n1), old).astype(jnp.bfloat16)
            for u in range(UNROLL):
                b = j * BLK_ROWS + g * UNROLL + u
                rel = pos[b] - base
                kb = kbuf[pl.ds(pl.multiple_of(b * per_row, per_row), per_row), :]
                vb = vbuf[pl.ds(pl.multiple_of(b * per_row, per_row), per_row), :]
                qb = qs[pl.ds(pl.multiple_of(b * HEAD_PAD, HEAD_PAD), HEAD_PAD), :].astype(jnp.bfloat16)
                s = lax.dot_general(qb, kb, (((1,), (1,)), ((), ())), preferred_element_type=jnp.float32) * scale
                valid = slot_rel <= rel
                s = jnp.where(valid, s, NEG)
                m = jnp.max(s, axis=-1, keepdims=True)
                w = jnp.where(valid, jnp.exp(s - m), 0.0)
                l = jnp.sum(w, axis=-1, keepdims=True)
                o = jnp.dot(w.astype(jnp.bfloat16), vb, preferred_element_type=jnp.float32)
                rs = pl.ds(pl.multiple_of(b * HEAD_PAD, HEAD_PAD), HEAD_PAD)
                osc[rs, :] = o
                msc[rs, :] = jnp.broadcast_to(m, (HEAD_PAD, hd))
                lsc[rs, :] = jnp.broadcast_to(l, (HEAD_PAD, hd))
            return 0
        lax.fori_loop(0, BLK_ROWS // UNROLL, b_body, 0)
        pltpu.make_async_copy(kbuf.at[sl], kc_out.at[sl], osem.at[2 * j]).start()
        pltpu.make_async_copy(vbuf.at[sl], vc_out.at[sl], osem.at[2 * j + 1]).start()
        return 0
    lax.fori_loop(0, n_blk, blk_body, 0)

    st = jnp.zeros((rows, hd), jnp.float32)
    for h in range(heads):
        o_out[:, h * hd:(h + 1) * hd] = osc[pl.ds(h, rows, stride=HEAD_PAD), :]
        st = jnp.where(lane == h, msc[pl.ds(h, rows, stride=HEAD_PAD), :], st)
        st = jnp.where(lane == HEAD_PAD + h, lsc[pl.ds(h, rows, stride=HEAD_PAD), :], st)
    o_out[:, heads * hd:] = st
    for j in range(n_blk):
        for c in c_out(j):
            c.wait()


def attn_call(pos, x, gain, wq, wk, wv, kc, vc, *, blk_len, heads, kv_loc):
    rows, dim = x.shape
    hd = LANES
    half = np.arange(hd) // 2
    freq = jnp.asarray((1.0 / (float(ROPE_THETA) ** (2.0 * half / hd))).astype(np.float32)).reshape(1, hd)
    n_k = dim // KCH
    n_blk = rows // BLK_ROWS
    crow = kc.shape[0]
    f32, bf = jnp.float32, jnp.bfloat16
    return pl.pallas_call(
        functools.partial(attn_kernel, blk_len=blk_len, heads=heads, kv_loc=kv_loc),
        out_shape=(jax.ShapeDtypeStruct((rows, heads * hd + LANES), f32), jax.ShapeDtypeStruct(kc.shape, bf),
                   jax.ShapeDtypeStruct(vc.shape, bf), jax.ShapeDtypeStruct((rows * kv_loc, hd), bf),
                   jax.ShapeDtypeStruct((rows * kv_loc, hd), bf)),
        in_specs=[pl.BlockSpec(memory_space=pltpu.SMEM), VM, VM, VM, ANY, ANY, ANY, ANY, ANY],
        out_specs=(VM, ANY, ANY, VM, VM),
        scratch_shapes=[
            pltpu.VMEM((rows, dim), bf), pltpu.VMEM(wq.shape, bf), pltpu.VMEM(wk.shape, bf), pltpu.VMEM(wv.shape, bf),
            pltpu.VMEM((rows, wq.shape[1] + 2 * wk.shape[1]), f32),
            pltpu.VMEM((crow, hd), bf), pltpu.VMEM((crow, hd), bf),
            pltpu.VMEM((rows, hd), f32), pltpu.VMEM((rows * HEAD_PAD, hd), f32),
            pltpu.VMEM((rows * kv_loc, hd), f32), pltpu.VMEM((rows * kv_loc, hd), f32),
            pltpu.VMEM((rows * HEAD_PAD, hd), f32), pltpu.VMEM((rows * HEAD_PAD, hd), f32),
            pltpu.VMEM((rows * HEAD_PAD, hd), f32),
            pltpu.SemaphoreType.DMA((n_k, 3)), pltpu.SemaphoreType.DMA((2 * n_blk,)),
            pltpu.SemaphoreType.DMA((2 * n_blk,)),
        ],
        compiler_params=pltpu.CompilerParams(vmem_limit_bytes=60 * 1024 * 1024),
        name='attn',
    )(pos, x, gain.reshape(-1, LANES), freq, wq, wk, wv, kc, vc)


MESH = pl.DeviceIdType.MESH
RING = 4
CORES = 2
PART_ROWS = 16
OWN_ROWS = 8


def tail_kernel(o_ref, x_hbm, gain_ref, wo, wg, wu, wd, out_ref,
                ring_g, ring_d, ra0, ma, ra1, ra2, of, ob, p1, rb1, rb2, hb, n2, ga, ua, ab, abf, p2, rd1, rd2, yb, xs,
                sem_g, sem_d, sem_x, send_a, recv_a, send_b, recv_b, send_c, recv_c, send_m, recv_m, send_d, recv_d,
                send_e, recv_e, *, heads, kc):
    f32, bf = jnp.float32, jnp.bfloat16
    hd = LANES
    ow = heads * hd
    half = wo.shape[1] // CORES
    quart = half // 2
    fh = wg.shape[1] // CORES
    n_g2 = ring_g.shape[0]
    n_d = ring_d.shape[0]
    n_wo = wo.shape[0] // kc
    n_k = wg.shape[0] // kc
    n_dn = wd.shape[0] // kc
    sp = lax.axis_index('sp')
    y = lax.axis_index('tp')
    x = lax.div(sp, CORES)
    c = lax.rem(sp, CORES)
    oc = 1 - c

    def xi(d):
        return lax.rem(x + (d + RING), RING)

    def yi(d):
        return lax.rem(y + (d + RING), RING)

    def xdev(d):
        return {'sp': xi(d) * CORES + c}

    def ydev(d):
        return {'tp': yi(d)}

    mate = {'sp': x * CORES + oc}

    pend = []

    def send(src, dst, ss, rs, dev):
        cp = pltpu.make_async_remote_copy(src_ref=src, dst_ref=dst, send_sem=ss, recv_sem=rs, device_id=dev, device_id_type=MESH)
        cp.start()
        pend.append(cp)

    def recv(dst, ss, rs):
        pltpu.make_async_remote_copy(src_ref=dst, dst_ref=dst, send_sem=ss, recv_sem=rs, device_id=mate, device_id_type=MESH).wait_recv()

    col_h = pl.multiple_of(c * half, half)
    col_f = pl.multiple_of(c * fh, fh)

    def g_copy(k, t):
        w = (wg, wu)[t]
        slot = lax.rem(k, n_g2)
        return pltpu.make_async_copy(w.at[pl.ds(pl.multiple_of(k * kc, kc), kc), pl.ds(col_f, fh)], ring_g.at[slot, t], sem_g.at[slot, t])

    def wo_copy(k):
        return pltpu.make_async_copy(wo.at[pl.ds(pl.multiple_of(k * kc, kc), kc), pl.ds(col_h, half)], ring_d.at[lax.rem(k, n_d)], sem_d.at[lax.rem(k, n_d)])

    def dn_copy(j):
        part = lax.div(j, n_dn // 2)
        row = lax.rem(c + part, 2) * fh + lax.rem(j, n_dn // 2) * kc
        slot = lax.rem(j + n_wo, n_d)
        return pltpu.make_async_copy(wd.at[pl.ds(pl.multiple_of(row, kc), kc), pl.ds(col_h, half)], ring_d.at[slot], sem_d.at[slot])

    barrier = pltpu.get_barrier_semaphore()
    for dev in (mate, xdev(1), xdev(-1), ydev(1), ydev(-1)):
        pl.semaphore_signal(barrier, inc=1, device_id=dev, device_id_type=MESH)
    row0 = x * (CORES * PART_ROWS) + lax.div(y, 2) * PART_ROWS
    x_copy = pltpu.make_async_copy(x_hbm.at[pl.ds(pl.multiple_of(row0, PART_ROWS), PART_ROWS), pl.ds(col_h, half)], xs, sem_x)
    x_copy.start()
    for k in range(min(n_wo, n_d)):
        wo_copy(k).start()
    pl.semaphore_wait(barrier, 5)

    for i, d in enumerate((2, 1, -1, 0)):
        send(o_ref.at[xi(d), oc], ra0.at[i], send_a.at[i], recv_a.at[i], mate)
    for k in range(n_g2):
        for t in range(2):
            g_copy(k, t).start()
    for j in range(n_d - n_wo):
        dn_copy(j).start()

    def merge(dst, a, b, r0, nr):
        rows = pl.ds(r0, nr)
        sa, sb = a[rows, pl.ds(ow, LANES)], b[rows, pl.ds(ow, LANES)]
        m = jnp.maximum(sa, sb)
        ea, eb = jnp.exp(sa - m), jnp.exp(sb - m)
        lane = lax.broadcasted_iota(jnp.int32, (nr, LANES), 1)
        l = sa * pltpu.roll(ea, HEAD_PAD, 1) + sb * pltpu.roll(eb, HEAD_PAD, 1)
        dst[rows, pl.ds(ow, LANES)] = jnp.where(lane < HEAD_PAD, m, l)
        for h in range(heads):
            hs = pl.ds(h * hd, hd)
            dst[rows, hs] = a[rows, hs] * ea[:, h:h + 1] + b[rows, hs] * eb[:, h:h + 1]

    R8 = OWN_ROWS
    lo, hi = pl.ds(0, R8), pl.ds(R8, R8)
    recv(ra0.at[0], send_a.at[0], recv_a.at[0])
    merge(ma.at[0], o_ref.at[xi(2), c], ra0.at[0], 0, 2 * R8)
    send(ma.at[0, lo], ra1.at[0], send_a.at[4], recv_a.at[4], xdev(1))
    send(ma.at[0, hi], ra1.at[1], send_a.at[5], recv_a.at[5], xdev(-1))
    recv(ra0.at[1], send_a.at[1], recv_a.at[1])
    merge(ma.at[1], o_ref.at[xi(1), c], ra0.at[1], 0, 2 * R8)
    send(ma.at[1, hi], ra2.at[0, hi], send_a.at[6], recv_a.at[6], xdev(1))
    recv(ra0.at[2], send_a.at[2], recv_a.at[2])
    merge(ma.at[2], o_ref.at[xi(-1), c], ra0.at[2], 0, 2 * R8)
    send(ma.at[2, lo], ra2.at[1, lo], send_a.at[7], recv_a.at[7], xdev(-1))
    recv(ra0.at[3], send_a.at[3], recv_a.at[3])
    merge(ma.at[3], o_ref.at[xi(0), c], ra0.at[3], 0, 2 * R8)
    recv(ra1.at[0], send_a.at[4], recv_a.at[4])
    merge(ma.at[4, lo], ma.at[1, lo], ra1.at[0], 0, R8)
    send(ma.at[4, lo], ra2.at[0, lo], send_a.at[8], recv_a.at[8], xdev(1))
    recv(ra1.at[1], send_a.at[5], recv_a.at[5])
    merge(ma.at[4, hi], ma.at[2, hi], ra1.at[1], 0, R8)
    send(ma.at[4, hi], ra2.at[1, hi], send_a.at[9], recv_a.at[9], xdev(-1))
    recv(ra2.at[0, hi], send_a.at[6], recv_a.at[6])
    recv(ra2.at[1, lo], send_a.at[7], recv_a.at[7])
    recv(ra2.at[0, lo], send_a.at[8], recv_a.at[8])
    merge(ma.at[5], ma.at[3], ra2.at[0], 0, 2 * R8)
    recv(ra2.at[1, hi], send_a.at[9], recv_a.at[9])
    merge(ma.at[6], ma.at[5], ra2.at[1], 0, 2 * R8)
    st = ma[6, :, ow:]
    for h in range(heads):
        hs = slice(h * hd, (h + 1) * hd)
        of[c, :, hs] = (ma[6, :, hs] / st[:, HEAD_PAD + h:HEAD_PAD + h + 1]).astype(bf).astype(f32)
    send(of.at[c], of.at[c], send_a.at[10], recv_a.at[10], mate)
    recv(of.at[oc], send_a.at[10], recv_a.at[10])
    for i in range(CORES):
        ob[i * PART_ROWS:(i + 1) * PART_ROWS, :] = of[i].astype(bf)

    p1[...] = jnp.zeros(p1.shape, f32)

    def wo_body(k, _):
        wo_copy(k).wait()
        p1[...] += jnp.dot(ob[:, pl.ds(pl.multiple_of(k * kc, kc), kc)], ring_d[lax.rem(k, n_d)], preferred_element_type=f32)

        @pl.when(k + n_d - n_wo < n_dn)
        def _():
            dn_copy(k + n_d - n_wo).start()
        return 0
    lax.fori_loop(0, n_wo, wo_body, 0)

    def rs_y(p, r1, r2, ss, rs):
        def blk(d, a):
            return p.at[pl.ds(pl.multiple_of(yi(d) * R8, R8), R8), pl.ds(a * quart, quart)]
        send(blk(2, 0), r1.at[0], ss.at[0], rs.at[0], ydev(1))
        send(blk(2, 1), r1.at[1], ss.at[1], rs.at[1], ydev(-1))
        ca, cb = pl.ds(0, quart), pl.ds(quart, quart)
        send(blk(1, 1), r2.at[0, :, cb], ss.at[2], rs.at[2], ydev(1))
        send(blk(-1, 0), r2.at[1, :, ca], ss.at[3], rs.at[3], ydev(-1))
        recv(r1.at[0], ss.at[0], rs.at[0])
        b = blk(1, 0)
        b[...] = b[...] + r1[0]
        send(b, r2.at[0, :, ca], ss.at[4], rs.at[4], ydev(1))
        recv(r1.at[1], ss.at[1], rs.at[1])
        b = blk(-1, 1)
        b[...] = b[...] + r1[1]
        send(b, r2.at[1, :, cb], ss.at[5], rs.at[5], ydev(-1))
        recv(r2.at[0, :, cb], ss.at[2], rs.at[2])
        recv(r2.at[1, :, ca], ss.at[3], rs.at[3])
        recv(r2.at[0, :, ca], ss.at[4], rs.at[4])
        recv(r2.at[1, :, cb], ss.at[5], rs.at[5])

    own = pl.ds(pl.multiple_of(y * R8, R8), R8)
    rs_y(p1, rb1, rb2, send_b, recv_b)
    x_copy.wait()
    xf = xs[...].astype(f32)
    x8 = jnp.where(lax.rem(y, 2) == 0, xf[:R8], xf[R8:])
    h8 = x8 + (p1[own, :] + rb2[0] + rb2[1])
    hb[c, y, :, 0:half] = h8
    hb[c, y, :, half:] = jnp.broadcast_to(jnp.sum(h8 * h8, axis=-1, keepdims=True), (R8, LANES))

    hw = half + LANES
    w0, w1 = pl.ds(0, quart), pl.ds(quart, hw - quart)
    send(hb.at[c, y], hb.at[c, y], send_c.at[0], recv_c.at[0], ydev(1))
    send(hb.at[c, y], hb.at[c, y], send_c.at[1], recv_c.at[1], ydev(-1))
    send(hb.at[c, y], hb.at[c, y], send_c.at[4], recv_c.at[4], mate)
    recv(hb.at[c, yi(-1)], send_c.at[0], recv_c.at[0])
    s = hb.at[c, yi(-1), :, w0]
    send(s, s, send_c.at[2], recv_c.at[2], ydev(1))
    send(hb.at[c, yi(-1)], hb.at[c, yi(-1)], send_c.at[5], recv_c.at[5], mate)
    recv(hb.at[c, yi(1)], send_c.at[1], recv_c.at[1])
    s = hb.at[c, yi(1), :, w1]
    send(s, s, send_c.at[3], recv_c.at[3], ydev(-1))
    send(hb.at[c, yi(1)], hb.at[c, yi(1)], send_c.at[6], recv_c.at[6], mate)
    recv(hb.at[c, yi(2), :, w0], send_c.at[2], recv_c.at[2])
    recv(hb.at[c, yi(2), :, w1], send_c.at[3], recv_c.at[3])
    send(hb.at[c, yi(2)], hb.at[c, yi(2)], send_c.at[7], recv_c.at[7], mate)
    for i, d in enumerate((0, -1, 1, 2)):
        recv(hb.at[oc, yi(d)], send_c.at[4 + i], recv_c.at[4 + i])
    gain = gain_ref[...].astype(f32)
    n_gr = half // LANES
    for g in range(RING // 2):
        hs = [jnp.concatenate([hb[i, 2 * g], hb[i, 2 * g + 1]], axis=0) for i in range(CORES)]
        ssq = hs[0][:, half:half + 1] + hs[1][:, half:half + 1]
        r = lax.rsqrt(ssq * (1.0 / (CORES * half)) + EPS)
        for i in range(CORES):
            gi = jnp.concatenate([gain[i * n_gr + j:i * n_gr + j + 1, :] for j in range(n_gr)], axis=1)
            n2[g * PART_ROWS:(g + 1) * PART_ROWS, i * half:(i + 1) * half] = (hs[i][:, :half] * r * gi).astype(bf)

    ga[...] = jnp.zeros(ga.shape, f32)
    ua[...] = jnp.zeros(ua.shape, f32)

    def g_body(k, _):
        slot = lax.rem(k, n_g2)
        lhs = n2[:, pl.ds(pl.multiple_of(k * kc, kc), kc)]
        g_copy(k, 0).wait()
        ga[...] += jnp.dot(lhs, ring_g[slot, 0], preferred_element_type=f32)
        g_copy(k, 1).wait()
        ua[...] += jnp.dot(lhs, ring_g[slot, 1], preferred_element_type=f32)

        @pl.when(k + n_g2 < n_k)
        def _():
            g_copy(k + n_g2, 0).start()
            g_copy(k + n_g2, 1).start()
        return 0
    lax.fori_loop(0, n_k, g_body, 0)
    gp = ga[...]
    act = (gp * jax.nn.sigmoid(gp) * ua[...]).astype(bf)
    ab[c] = act.astype(f32)
    send(ab.at[c], ab.at[c], send_m.at[0], recv_m.at[0], mate)
    abf[:, 0:fh] = act
    p2[...] = jnp.zeros(p2.shape, f32)

    def dn_step(j):
        dn_copy(j).wait()
        p2[...] += jnp.dot(abf[:, pl.ds(pl.multiple_of(j * kc, kc), kc)], ring_d[lax.rem(j + n_wo, n_d)], preferred_element_type=f32)

        @pl.when(j + n_d < n_dn)
        def _():
            dn_copy(j + n_d).start()
        return 0
    lax.fori_loop(0, n_dn // 2, lambda j, _: dn_step(j), 0)
    recv(ab.at[oc], send_m.at[0], recv_m.at[0])
    abf[:, fh:] = ab[oc].astype(bf)
    lax.fori_loop(n_dn // 2, n_dn, lambda j, _: dn_step(j), 0)

    rs_y(p2, rd1, rd2, send_d, recv_d)
    y8 = hb[c, y, :, 0:half] + (p2[own, :] + rd2[0] + rd2[1])

    def at(dp, dq):
        return (lax.rem(x + (dp * oc + dq * c) + 2 * RING, RING), lax.rem(y + (dp * c + dq * oc) + 2 * RING, RING))

    def piece(core, dp, dq, cols=None):
        xx, yy = at(dp, dq)
        return yb.at[core, xx, yy] if cols is None else yb.at[core, xx, yy, :, cols]

    def pdev(d):
        xx, yy = at(d, 0)
        return {'sp': xx * CORES + c, 'tp': yy}

    def qdev(d):
        xx, yy = at(0, d)
        return {'sp': xx * CORES + c, 'tp': yy}

    cnt = [0]

    def rsem(dp, dq, hf):
        return recv_e.at[((dp % RING) * RING + (dq % RING)) * 2 + hf]

    def esend(dp, dq, dev, rp, rq, hf, cols=None):
        v = piece(c, dp, dq, cols)
        send(v, v, send_e.at[cnt[0]], rsem(rp, rq, hf), dev)
        cnt[0] += 1

    def erecv(dp, dq, hf, cols=None):
        recv(piece(c, dp, dq, cols), send_e.at[0], rsem(dp, dq, hf))

    order_p = (0, -1, 1, 2)
    ca, cb = pl.ds(0, quart), pl.ds(quart, quart)

    def to_mate(dp, dq):
        v = piece(c, dp, dq)
        send(v, v, send_e.at[cnt[0]], recv_e.at[2 * RING * RING + (dp % RING) * RING + (dq % RING)], mate)
        cnt[0] += 1

    def q_send(dp):
        esend(dp, 0, qdev(1), dp, -1, 0)
        esend(dp, 0, qdev(-1), dp, 1, 0)

    def q_fwd(dp):
        erecv(dp, -1, 0)
        esend(dp, -1, qdev(1), dp, -2, 0, ca)
        to_mate(dp, -1)
        erecv(dp, 1, 0)
        esend(dp, 1, qdev(-1), dp, 2, 1, cb)
        to_mate(dp, 1)

    xx, yy = at(0, 0)
    yb[c, xx, yy] = y8.astype(bf).astype(f32)
    esend(0, 0, pdev(1), -1, 0, 0)
    esend(0, 0, pdev(-1), 1, 0, 0)
    q_send(0)
    to_mate(0, 0)
    erecv(-1, 0, 0)
    esend(-1, 0, pdev(1), -2, 0, 0, ca)
    q_send(-1)
    to_mate(-1, 0)
    erecv(1, 0, 0)
    esend(1, 0, pdev(-1), 2, 0, 1, cb)
    q_send(1)
    to_mate(1, 0)
    q_fwd(0)
    erecv(2, 0, 0, ca)
    erecv(2, 0, 1, cb)
    q_send(2)
    to_mate(2, 0)
    q_fwd(-1)
    q_fwd(1)
    q_fwd(2)
    for dp in order_p:
        erecv(dp, 2, 0, ca)
        erecv(dp, 2, 1, cb)
        to_mate(dp, 2)
    for dp in order_p:
        for dq in (0, -1, 1, 2):
            xx = lax.rem(x + (dp * c + dq * oc) + 2 * RING, RING)
            yy = lax.rem(y + (dp * oc + dq * c) + 2 * RING, RING)
            recv(yb.at[oc, xx, yy], send_e.at[0], recv_e.at[2 * RING * RING + (dp % RING) * RING + (dq % RING)])
    for xx in range(RING):
        for g in range(RING // 2):
            r0 = xx * CORES * PART_ROWS + g * PART_ROWS
            for i in range(CORES):
                v = jnp.concatenate([yb[i, xx, 2 * g], yb[i, xx, 2 * g + 1]], axis=0)
                out_ref[r0:r0 + PART_ROWS, i * half:(i + 1) * half] = v.astype(bf)
    for cp in pend:
        cp.wait_send()


def tail_call(part, x, gain, wo, wg, wu, wd, *, heads, kc, n_g2, n_d):
    rows, dim = x.shape
    f32, bf = jnp.float32, jnp.bfloat16
    sw = heads * LANES + LANES
    half, fh = dim // CORES, wg.shape[1] // CORES
    chip_rows = CORES * PART_ROWS
    D = pltpu.SemaphoreType.DMA
    V = pltpu.VMEM
    n_e = 2 * RING * RING + RING * RING
    return pl.pallas_call(
        functools.partial(tail_kernel, heads=heads, kc=kc),
        out_shape=jax.ShapeDtypeStruct((rows, dim), bf),
        in_specs=[VM, ANY, VM, ANY, ANY, ANY, ANY],
        out_specs=VM,
        scratch_shapes=[
            V((n_g2, 2, kc, fh), bf), V((n_d, kc, half), bf),
            V((RING, PART_ROWS, sw), f32), V((7, PART_ROWS, sw), f32), V((2, OWN_ROWS, sw), f32), V((2, PART_ROWS, sw), f32),
            V((CORES, PART_ROWS, heads * LANES), f32), V((chip_rows, heads * LANES), bf),
            V((chip_rows, half), f32), V((2, OWN_ROWS, half // 2), f32), V((2, OWN_ROWS, half), f32),
            V((CORES, RING, OWN_ROWS, half + LANES), f32), V((chip_rows, dim), bf),
            V((chip_rows, fh), f32), V((chip_rows, fh), f32), V((CORES, chip_rows, fh), f32), V((chip_rows, CORES * fh), bf),
            V((chip_rows, half), f32), V((2, OWN_ROWS, half // 2), f32), V((2, OWN_ROWS, half), f32),
            V((CORES, RING, RING, OWN_ROWS, half), f32), V((PART_ROWS, half), bf),
            D((n_g2, 2)), D((n_d,)), D(()), D((11,)), D((11,)), D((6,)), D((6,)), D((8,)), D((8,)), D((1,)), D((1,)), D((6,)), D((6,)),
            D((40,)), D((n_e,)),
        ],
        compiler_params=pltpu.CompilerParams(vmem_limit_bytes=67043328, collective_id=0, has_side_effects=True),
        name='tail',
    )(part.reshape(rows // chip_rows, CORES, PART_ROWS, sw), x, gain.reshape(-1, LANES), wo, wg, wu, wd)


def solution(mesh):
    def local_step(layer_in, new_pos, k_blk, v_blk, attn_gain, w_query, w_key, w_value, w_out, mlp_gain, w_gate, w_up, w_down):
        num_rows = layer_in.shape[0]
        blk_len, kv_loc, head_dim = k_blk.shape[1:]
        heads = w_query.shape[1] // head_dim
        flat = (num_rows * blk_len * kv_loc, head_dim)
        part, k_upd, v_upd, k_new, v_new = attn_call(
            new_pos, layer_in, attn_gain, w_query, w_key, w_value, k_blk.reshape(flat), v_blk.reshape(flat),
            blk_len=blk_len, heads=heads, kv_loc=kv_loc)
        layer_out = tail_call(part, layer_in, mlp_gain, w_out, w_gate, w_up, w_down, heads=heads, kc=512, n_g2=8, n_d=5)
        new_shape = (num_rows, kv_loc, head_dim)
        return layer_out, k_upd.reshape(k_blk.shape), v_upd.reshape(v_blk.shape), k_new.reshape(new_shape), v_new.reshape(new_shape)

    cache_spec = P('dp', 'sp', 'tp', None)
    new_spec = P('dp', 'tp', None)
    in_specs = (P('dp', None), P('dp'), cache_spec, cache_spec, P(None), P(None, 'tp'), P(None, 'tp'), P(None, 'tp'), P('tp', None), P(None), P(None, 'tp'), P(None, 'tp'), P('tp', None))
    out_specs = (P('dp', None), cache_spec, cache_spec, new_spec, new_spec)
    return jax.shard_map(local_step, mesh=mesh, in_specs=in_specs, out_specs=out_specs, check_vma=False)
```
